32 devices in a mesh: dp: 2 (over x), col: 4 (over z), row: 4 (over y, core).
Axes of the slice: x: 2, y: 2, z: 4, core: 2. Of those that a mesh axis runs over, the one named last changes fastest.
Arguments:
- x_in: bfloat16 [2, 2048, 6144], P(None, ('dp', 'row'), 'col'), parts along dimension 1
- ln_gamma: float32 [6144], P('col')
- w_in: bfloat16 [6144, 24576], P('row', 'col')
- w_out: bfloat16 [24576, 6144], P('row', 'col')
Outputs:
- output: bfloat16 [2, 2048, 6144], P(None, ('dp', 'row'), 'col'), parts along dimension 1
There are 2 independent parts. The reference program is written for one: setup_inputs(seed, part) draws one part's arguments, and reference() takes and returns one part's arrays. A program takes and returns all parts, laid end to end along the dimension named above; an argument that names none is the same for every part.
All inputs are finite; a program needn't handle non-finite values.
Results may differ from the reference program's by a relative error of at most 0.001.
Values are sent between devices in bfloat16 or wider.
A program may use at most 1 GiB of HBM per device.

```python
import jax
import jax.numpy as jnp
from jax import lax

D_MODEL = 6144
D_FF = 24576
MB_TOKENS = 1024
ROW_BLOCK = 256
LN_EPS = 1e-5
N_BLOCKS = 2 * MB_TOKENS // ROW_BLOCK


def setup_inputs(seed: int = 0, part: int = 0) -> dict:
    base_key = jax.random.key(seed)
    part_key = jax.random.fold_in(base_key, part)
    key_noise, key_off, key_tilt, key_col = jax.random.split(part_key, 4)
    shared_key = jax.random.key(seed + 1)
    key_gamma, key_win, key_wout = jax.random.split(shared_key, 3)
    ramp = jnp.arange(D_MODEL, dtype=jnp.float32) / D_MODEL
    col_scale = (0.4 + 1.2 * ramp) * jax.random.uniform(key_col, (D_MODEL,), jnp.float32, 0.8, 1.2)
    noise = jax.random.normal(key_noise, (2, MB_TOKENS, D_MODEL), jnp.float32)
    row_off = 0.5 * jax.random.normal(key_off, (2, MB_TOKENS, 1), jnp.float32)
    row_tilt = jax.random.normal(key_tilt, (2, MB_TOKENS, 1), jnp.float32)
    x_val = row_off + row_tilt * (ramp - 0.5) + col_scale * noise
    ln_gamma = jax.random.uniform(key_gamma, (D_MODEL,), jnp.float32, 0.5, 1.5)
    w_in = jax.random.normal(key_win, (D_MODEL, D_FF), jnp.float32) * D_MODEL ** -0.5
    w_out = jax.random.normal(key_wout, (D_FF, D_MODEL), jnp.float32) * (1.5 * D_FF ** -0.5)
    return {"x_in": x_val.astype(jnp.bfloat16), "ln_gamma": ln_gamma, "w_in": w_in.astype(jnp.bfloat16), "w_out": w_out.astype(jnp.bfloat16)}


def reference(x_in, ln_gamma, w_in, w_out):
    row_blocks = x_in.reshape(N_BLOCKS, ROW_BLOCK, D_MODEL)

    def one_block(x_blk):
        x_f32 = x_blk.astype(jnp.float32)
        row_mean = jnp.sum(x_f32, axis=-1, keepdims=True) / D_MODEL
        row_var = jnp.sum(x_f32 * x_f32, axis=-1, keepdims=True) / D_MODEL - row_mean * row_mean
        z_norm = ((x_f32 - row_mean) * lax.rsqrt(row_var + LN_EPS) * ln_gamma).astype(jnp.bfloat16)
        hidden = jnp.dot(z_norm, w_in, preferred_element_type=jnp.float32)
        hidden = jax.nn.gelu(hidden, approximate=True).astype(jnp.bfloat16)
        branch = jnp.dot(hidden, w_out, preferred_element_type=jnp.float32)
        return (x_f32 + branch).astype(jnp.bfloat16)

    return lax.map(one_block, row_blocks).reshape(2, MB_TOKENS, D_MODEL)
```

```python
import functools

import jax
import jax.numpy as jnp
from jax import lax
from jax.experimental import pallas as pl
from jax.experimental.pallas import tpu as pltpu
from jax.sharding import PartitionSpec as P

LN_EPS = 1e-5
MESH = pl.DeviceIdType.MESH
NCHUNK = 6
LN_ROWS = 16


def _kernel(
    x_ref, gamma_ref, w1_ref, w2_ref,
    y_ref, w1g, w2g, hg,
    xg, zv, gg, wbuf, hst, acc, hin, w2in, part, xres,
    ys, yr, xs, xr, ps, pr,
    xsu, xsd, xrecv, xps, xpr, gs, gr, hsu, hsd, hrecv, fs, fr,
    lsem, wsem, hsem, msem,
):
    dp, z, row = lax.axis_index("dp"), lax.axis_index("col"), lax.axis_index("row")
    yy, c = row // 2, row % 2
    tok, dblk = x_ref.shape
    toks = 2 * tok
    rows1, fz = w1_ref.shape
    fhalf = fz // 2
    nc = fhalf // NCHUNK
    half1, half2 = rows1 // 2, nc // 2
    nt = wbuf.shape[2]
    d_model = 4 * dblk

    partner = (dp, z, 2 * yy + (1 - c))
    xnb = (1 - dp, z, row)
    ynb = [(dp, z, 2 * (1 - yy) + ct) for ct in range(2)]
    up = (dp, jnp.minimum(z + 1, 3), row)
    dn = (dp, jnp.maximum(z - 1, 0), row)
    zoth = [(dp, (z + k) % 4, row) for k in range(1, 4)]

    def rcopy(src, dst, ssem, rsem, dev):
        return pltpu.make_async_remote_copy(
            src_ref=src, dst_ref=dst, send_sem=ssem, recv_sem=rsem, device_id=dev, device_id_type=MESH)

    def y_desc(w, j, ct):
        if w == 0:
            src = w1_ref.at[pl.ds(dp * half1, half1), pl.ds(ct * fhalf + j * nc, nc)]
            dst = w1g.at[j, row, pl.ds(dp * half1, half1), :]
        else:
            src = w2_ref.at[pl.ds(ct * fhalf + j * nc + dp * half2, half2), :]
            dst = w2g.at[row, j, pl.ds(dp * half2, half2), :]
        return rcopy(src, dst, ys.at[w, j, ct], yr.at[w, j, c], ynb[ct])

    def region(w, j, cs, side):
        rr = 2 * (1 - yy) + cs
        if w == 0:
            return w1g.at[j, rr, pl.ds(side * half1, half1), :]
        return w2g.at[rr, j, pl.ds(side * half2, half2), :]

    def y_arrive_forward(w, j):
        for cs in range(2):
            reg = region(w, j, cs, dp)
            rcopy(reg, reg, ys.at[w, j, cs], yr.at[w, j, cs], ynb[cs]).wait_recv()
            rcopy(reg, reg, xs.at[w, j, cs], xr.at[w, j, cs], xnb).start()

    def x_arrive(w, j):
        for cs in range(2):
            reg = region(w, j, cs, 1 - dp)
            rcopy(reg, reg, xs.at[w, j, cs], xr.at[w, j, cs], xnb).wait_recv()

    def x_sent(w, j):
        for cs in range(2):
            reg = region(w, j, cs, dp)
            rcopy(reg, reg, xs.at[w, j, cs], xr.at[w, j, cs], xnb).wait_send()

    def p_desc(w, j):
        if w == 0:
            src = w1_ref.at[:, pl.ds((1 - c) * fhalf + j * nc, nc)]
            dst = w1g.at[j, row]
        else:
            src = w2_ref.at[pl.ds((1 - c) * fhalf + j * nc, nc), :]
            dst = w2g.at[row, j]
        return rcopy(src, dst, ps.at[w, j], pr.at[w, j], partner)

    def p_arrive(w, j):
        rp = 2 * yy + (1 - c)
        dst = w1g.at[j, rp] if w == 0 else w2g.at[rp, j]
        rcopy(dst, dst, ps.at[w, j], pr.at[w, j], partner).wait_recv()

    def x_blk(zz):
        return xg.at[zz, pl.ds(c * tok, tok), :]

    def x_up(zz, src=None):
        return rcopy(x_blk(zz) if src is None else src, x_blk(zz), xsu.at[zz], xrecv.at[zz], up)

    def x_dn(zz, src=None):
        return rcopy(x_blk(zz) if src is None else src, x_blk(zz), xsd.at[zz], xrecv.at[zz], dn)

    def x_part(zz, src=None):
        return rcopy(x_blk(zz) if src is None else src, x_blk(zz), xps.at[zz], xpr.at[zz], partner)

    def h_up(zz, j):
        return rcopy(hg.at[zz, j], hg.at[zz, j], hsu.at[zz, j], hrecv.at[zz, j], up)

    def h_dn(zz, j):
        return rcopy(hg.at[zz, j], hg.at[zz, j], hsd.at[zz, j], hrecv.at[zz, j], dn)

    barrier = pltpu.get_barrier_semaphore()
    peers = [partner, xnb] + ynb + zoth
    for dev in peers:
        pl.semaphore_signal(barrier, inc=1, device_id=dev, device_id_type=MESH)
    pl.semaphore_wait(barrier, len(peers))

    @pl.when(z < 3)
    def _():
        x_up(z, x_ref).start()

    @pl.when(z > 0)
    def _():
        x_dn(z, x_ref).start()

    x_part(z, x_ref).start()
    own_x = pltpu.make_async_copy(x_ref, x_blk(z), lsem.at[0])
    own_x.start()
    res_x = pltpu.make_async_copy(x_ref, xres, lsem.at[1])
    res_x.start()
    own_g = pltpu.make_async_copy(gamma_ref, gg.at[z], lsem.at[2])
    own_g.start()
    for k in range(3):
        rcopy(gamma_ref, gg.at[z], gs.at[k], gr.at[z], zoth[k]).start()

    def start_w(w):
        def body(j, _):
            p_desc(w, j).start()
            for ct in range(2):
                y_desc(w, j, ct).start()
            return 0
        lax.fori_loop(0, NCHUNK, body, 0)

    start_w(0)

    def zero(i, _):
        acc[pl.ds(i * 64, 64), :] = jnp.zeros((64, acc.shape[1]), jnp.float32)
        return 0
    lax.fori_loop(0, toks // 64, zero, 0)

    def hop(h, desc_up, desc_dn, extra=None):
        @pl.when(z >= h)
        def _():
            desc_up(z - h).wait_recv()

            @pl.when(z < 3)
            def _():
                desc_up(z - h).start()
            if extra is not None:
                extra(z - h)

        @pl.when(z + h <= 3)
        def _():
            desc_dn(z + h).wait_recv()

            @pl.when(z > 0)
            def _():
                desc_dn(z + h).start()
            if extra is not None:
                extra(z + h)

    for h in (1, 2, 3):
        hop(h, x_up, x_dn, lambda zz: x_part(zz).start())
        y_arrive_forward(0, h - 1)

    for zz in range(4):
        blk = xg.at[zz, pl.ds((1 - c) * tok, tok), :]
        rcopy(blk, blk, xps.at[zz], xpr.at[zz], partner).wait_recv()
    own_x.wait()
    own_g.wait()
    res_x.wait()
    for k in range(3):
        zo = (z + k + 1) % 4
        rcopy(gg.at[zo], gg.at[zo], gs.at[k], gr.at[zo], zoth[k]).wait_recv()

    def norm(i, _):
        rs = pl.ds(pl.multiple_of(i * LN_ROWS, LN_ROWS), LN_ROWS)
        s1 = jnp.zeros((LN_ROWS, 1), jnp.float32)
        s2 = jnp.zeros((LN_ROWS, 1), jnp.float32)
        for q in range(4):
            v = xg[q, rs, :].astype(jnp.float32)
            s1 += jnp.sum(v, axis=-1, keepdims=True)
            s2 += jnp.sum(v * v, axis=-1, keepdims=True)
        mean = s1 / d_model
        inv = lax.rsqrt(s2 / d_model - mean * mean + LN_EPS)
        for q in range(4):
            v = xg[q, rs, :].astype(jnp.float32)
            g = gg[q, 0:1, :]
            zv[rs, q * dblk:(q + 1) * dblk] = ((v - mean) * inv * g).astype(jnp.bfloat16)
        return 0
    lax.fori_loop(0, toks // LN_ROWS, norm, 0)

    start_w(1)

    def w1_loads(j, s):
        out = []
        for k in range(4):
            rr = (row + k) % 4
            dst = wbuf.at[s, pl.ds(rr * rows1, rows1), :]
            if k == 0:
                src = w1_ref.at[:, pl.ds(c * fhalf + j * nc + s * nt, nt)]
            else:
                src = w1g.at[j, rr, :, pl.ds(s * nt, nt)]
            out.append(pltpu.make_async_copy(src, dst, wsem.at[s, k]))
        return out

    def mat1(j, _):
        @pl.when(j == 3)
        def _():
            y_arrive_forward(0, 3)
            y_arrive_forward(0, 4)

        @pl.when(j == 4)
        def _():
            y_arrive_forward(0, 5)

        p_arrive(0, j)
        x_arrive(0, j)
        for s in range(nc // nt):
            for cp in w1_loads(j, s):
                cp.start()
        for s in range(nc // nt):
            for cp in w1_loads(j, s):
                cp.wait()

            def mtile(m, _):
                ms = pl.ds(pl.multiple_of(m * 512, 512), 512)
                u = jnp.dot(zv[ms, :], wbuf[s], preferred_element_type=jnp.float32)
                hst[ms, s * nt:(s + 1) * nt] = jax.nn.gelu(u, approximate=True).astype(jnp.bfloat16)
                return 0
            lax.fori_loop(0, toks // 512, mtile, 0)
        st = pltpu.make_async_copy(hst, hg.at[z, j], hsem.at[0])
        st.start()
        st.wait()

        @pl.when(z < 3)
        def _():
            h_up(z, j).start()

        @pl.when(z > 0)
        def _():
            h_dn(z, j).start()
        return 0
    lax.fori_loop(0, NCHUNK, mat1, 0)

    def w2_load(zz, j, s):
        dst = w2in.at[s]

        @pl.when(zz == row)
        def _():
            pltpu.make_async_copy(w2_ref.at[pl.ds(c * fhalf + j * nc, nc), :], dst, msem.at[s, 0]).start()

        @pl.when(zz != row)
        def _():
            pltpu.make_async_copy(w2g.at[zz, j], dst, msem.at[s, 0]).start()

    def mat2(pair, j):
        for s in range(2):
            w2_load(pair[s], j, s)
            pltpu.make_async_copy(hg.at[pair[s], j], hin.at[s], msem.at[s, 1]).start()
        for s in range(2):
            pltpu.make_async_copy(w2g.at[pair[s], j], w2in.at[s], msem.at[s, 0]).wait()
            pltpu.make_async_copy(hg.at[pair[s], j], hin.at[s], msem.at[s, 1]).wait()

            def mtile(m, _):
                ms = pl.ds(pl.multiple_of(m * 256, 256), 256)
                acc[ms, :] += jnp.dot(hin[s, ms, :], w2in[s], preferred_element_type=jnp.float32)
                return 0
            lax.fori_loop(0, toks // 256, mtile, 0)

    pair_a = (z, z + 1 - 2 * (z % 2))
    zb = (z + 2) % 4
    pair_b = (zb, zb + 1 - 2 * (zb % 2))

    def b1(j, _):
        hop(1, lambda zz: h_up(zz, j), lambda zz: h_dn(zz, j))
        return 0
    lax.fori_loop(0, NCHUNK, b1, 0)
    y_arrive_forward(1, 0)

    def b2(j, _):
        hop(2, lambda zz: h_up(zz, j), lambda zz: h_dn(zz, j))

        @pl.when(j < NCHUNK - 1)
        def _():
            y_arrive_forward(1, jnp.minimum(j + 1, NCHUNK - 1))
        p_arrive(1, j)
        x_arrive(1, j)
        mat2(pair_a, j)
        return 0
    lax.fori_loop(0, NCHUNK, b2, 0)

    def b3(j, _):
        hop(3, lambda zz: h_up(zz, j), lambda zz: h_dn(zz, j))
        mat2(pair_b, j)
        return 0
    lax.fori_loop(0, NCHUNK, b3, 0)

    fin = rcopy(acc.at[pl.ds((1 - c) * tok, tok), :], part, fs, fr, partner)
    fin.start()
    fin.wait()

    def final(i, _):
        rs = pl.ds(pl.multiple_of(i * 64, 64), 64)
        own = acc[pl.ds(pl.multiple_of(c * tok + i * 64, 64), 64), :]
        y_ref[rs, :] = (xres[rs, :].astype(jnp.float32) + (own + part[rs, :])).astype(jnp.bfloat16)
        return 0
    lax.fori_loop(0, tok // 64, final, 0)

    for w in range(2):
        def drain(j, _):
            p_desc(w, j).wait_send()
            for ct in range(2):
                y_desc(w, j, ct).wait_send()
            x_sent(w, j)
            return 0
        lax.fori_loop(0, NCHUNK, drain, 0)
    for k in range(3):
        rcopy(gamma_ref, gg.at[z], gs.at[k], gr.at[z], zoth[k]).wait_send()

    def drain_z(zz, _):
        x_part(zz).wait_send()

        @pl.when(jnp.logical_and(zz <= z, z < 3))
        def _():
            x_up(zz).wait_send()

            def d(j, _):
                h_up(zz, j).wait_send()
                return 0
            lax.fori_loop(0, NCHUNK, d, 0)

        @pl.when(jnp.logical_and(zz >= z, z > 0))
        def _():
            x_dn(zz).wait_send()

            def d(j, _):
                h_dn(zz, j).wait_send()
                return 0
            lax.fori_loop(0, NCHUNK, d, 0)
        return 0
    lax.fori_loop(0, 4, drain_z, 0)


def solution(mesh):
    act_spec = P(None, ("dp", "row"), "col")

    def per_device(x_blk, gamma_blk, w_in_blk, w_out_blk):
        mb, rows, dblk = x_blk.shape
        tok = mb * rows
        fz = w_in_blk.shape[1]
        fhalf = fz // 2
        nc = fhalf // NCHUNK
        bf16, f32 = jnp.bfloat16, jnp.float32
        x2 = x_blk.reshape(tok, dblk)
        g2 = jnp.broadcast_to(gamma_blk[None, :], (8, dblk))
        dma = pltpu.SemaphoreType.DMA
        anyspec = pl.BlockSpec(memory_space=pl.ANY)
        out = pl.pallas_call(
            _kernel,
            out_shape=(
                jax.ShapeDtypeStruct((tok, dblk), bf16),
                jax.ShapeDtypeStruct((NCHUNK, 4, w_in_blk.shape[0], nc), bf16),
                jax.ShapeDtypeStruct((4, NCHUNK, nc, dblk), bf16),
                jax.ShapeDtypeStruct((4, NCHUNK, 2 * tok, nc), bf16),
            ),
            in_specs=[anyspec] * 4,
            out_specs=(pl.BlockSpec(memory_space=pltpu.VMEM), anyspec, anyspec, anyspec),
            scratch_shapes=[
                pltpu.VMEM((4, 2 * tok, dblk), bf16),
                pltpu.VMEM((2 * tok, 4 * dblk), bf16),
                pltpu.VMEM((4, 8, dblk), f32),
                pltpu.VMEM((2, 4 * dblk, 256), bf16),
                pltpu.VMEM((2 * tok, nc), bf16),
                pltpu.VMEM((2 * tok, dblk), f32),
                pltpu.VMEM((2, 2 * tok, nc), bf16),
                pltpu.VMEM((2, nc, dblk), bf16),
                pltpu.VMEM((tok, dblk), f32),
                pltpu.VMEM((tok, dblk), bf16),
                dma((2, NCHUNK, 2)), dma((2, NCHUNK, 2)), dma((2, NCHUNK, 2)), dma((2, NCHUNK, 2)),
                dma((2, NCHUNK)), dma((2, NCHUNK)),
                dma((4,)), dma((4,)), dma((4,)), dma((4,)), dma((4,)), dma((3,)), dma((4,)),
                dma((4, NCHUNK)), dma((4, NCHUNK)), dma((4, NCHUNK)), dma, dma,
                dma((3,)), dma((2, 4)), dma((1,)), dma((2, 2)),
            ],
            compiler_params=pltpu.CompilerParams(
                collective_id=0, has_side_effects=True, vmem_limit_bytes=66_000_000),
            name="mlp",
        )(x2, g2, w_in_blk, w_out_blk)
        return out[0].reshape(mb, rows, dblk)

    return jax.shard_map(
        per_device, mesh=mesh, in_specs=(act_spec, P("col"), P("row", "col"), P("row", "col")),
        out_specs=act_spec, check_vma=False)
```

```python
import functools

import jax
import jax.numpy as jnp
from jax import lax
from jax.experimental import pallas as pl
from jax.experimental.pallas import tpu as pltpu
from jax.sharding import PartitionSpec as P

LN_EPS = 1e-5
MESH = pl.DeviceIdType.MESH
NCHUNK = 6
LN_ROWS = 16


def _kernel(
    x_ref, gamma_ref, w1_ref, w2_ref,
    y_ref, w1g, w2g, hg, w2x,
    xg, zv, gg, wbuf, hst, acc, accx, hin, w2in, part, partx, parte, xres,
    ys, yr, xs, xr, ps, pr,
    xsu, xsd, xrecv, xps, xpr, gs, gr, hsu, hsd, hrecv, fs, fr,
    wxs, wxr, pxs, pxr, pes, per,
    lsem, wsem, hsem, msem,
):
    dp, z, row = lax.axis_index("dp"), lax.axis_index("col"), lax.axis_index("row")
    yy, c = row // 2, row % 2
    tok, dblk = x_ref.shape
    toks = 2 * tok
    rows1, fz = w1_ref.shape
    fhalf = fz // 2
    nc = fhalf // NCHUNK
    half1, half2 = rows1 // 2, nc // 2
    nt = wbuf.shape[2]
    d_model = 4 * dblk

    partner = (dp, z, 2 * yy + (1 - c))
    xnb = (1 - dp, z, row)
    ynb = [(dp, z, 2 * (1 - yy) + ct) for ct in range(2)]
    up = (dp, jnp.minimum(z + 1, 3), row)
    dn = (dp, jnp.maximum(z - 1, 0), row)
    zoth = [(dp, (z + k) % 4, row) for k in range(1, 4)]
    zoth2 = [(dp, (z + k) % 4, 2 * yy + (1 - c)) for k in range(1, 4)]
    mbt = tok // 2
    hrow = 2 * mbt
    end = jnp.logical_or(z == 0, z == 3)
    inner = jnp.logical_not(end)
    moved = 1 + yy
    z_in = jnp.where(z < 2, 1, 2)
    z_end = jnp.where(z < 2, 0, 3)

    def rcopy(src, dst, ssem, rsem, dev):
        return pltpu.make_async_remote_copy(
            src_ref=src, dst_ref=dst, send_sem=ssem, recv_sem=rsem, device_id=dev, device_id_type=MESH)

    def y_desc(w, j, ct):
        if w == 0:
            src = w1_ref.at[pl.ds(dp * half1, half1), pl.ds(ct * fhalf + j * nc, nc)]
            dst = w1g.at[j, row, pl.ds(dp * half1, half1), :]
        else:
            src = w2_ref.at[pl.ds(ct * fhalf + j * nc + dp * half2, half2), :]
            dst = w2g.at[row, j, pl.ds(dp * half2, half2), :]
        return rcopy(src, dst, ys.at[w, j, ct], yr.at[w, j, c], ynb[ct])

    def region(w, j, cs, side):
        rr = 2 * (1 - yy) + cs
        if w == 0:
            return w1g.at[j, rr, pl.ds(side * half1, half1), :]
        return w2g.at[rr, j, pl.ds(side * half2, half2), :]

    def y_arrive_forward(w, j):
        for cs in range(2):
            reg = region(w, j, cs, dp)
            rcopy(reg, reg, ys.at[w, j, cs], yr.at[w, j, cs], ynb[cs]).wait_recv()
            rcopy(reg, reg, xs.at[w, j, cs], xr.at[w, j, cs], xnb).start()

    def x_arrive(w, j):
        for cs in range(2):
            reg = region(w, j, cs, 1 - dp)
            rcopy(reg, reg, xs.at[w, j, cs], xr.at[w, j, cs], xnb).wait_recv()

    def x_sent(w, j):
        for cs in range(2):
            reg = region(w, j, cs, dp)
            rcopy(reg, reg, xs.at[w, j, cs], xr.at[w, j, cs], xnb).wait_send()

    def p_desc(w, j):
        if w == 0:
            src = w1_ref.at[:, pl.ds((1 - c) * fhalf + j * nc, nc)]
            dst = w1g.at[j, row]
        else:
            src = w2_ref.at[pl.ds((1 - c) * fhalf + j * nc, nc), :]
            dst = w2g.at[row, j]
        return rcopy(src, dst, ps.at[w, j], pr.at[w, j], partner)

    def p_arrive(w, j):
        rp = 2 * yy + (1 - c)
        dst = w1g.at[j, rp] if w == 0 else w2g.at[rp, j]
        rcopy(dst, dst, ps.at[w, j], pr.at[w, j], partner).wait_recv()

    def x_blk(zz, m):
        return xg.at[zz, pl.ds(m * hrow + c * mbt, mbt), :]

    def x_src(m):
        return x_ref.at[pl.ds(m * mbt, mbt), :]

    def x_up(zz, m, src=None):
        return rcopy(x_blk(zz, m) if src is None else src, x_blk(zz, m), xsu.at[zz, m], xrecv.at[zz, m], up)

    def x_dn(zz, m, src=None):
        return rcopy(x_blk(zz, m) if src is None else src, x_blk(zz, m), xsd.at[zz, m], xrecv.at[zz, m], dn)

    def x_part(zz, m, src=None):
        return rcopy(x_blk(zz, m) if src is None else src, x_blk(zz, m), xps.at[zz, m], xpr.at[zz, m], partner)

    def h_blk(zz, j, m):
        return hg.at[zz, j, pl.ds(m * hrow, hrow), :]

    def h_up(zz, j, m):
        return rcopy(h_blk(zz, j, m), h_blk(zz, j, m), hsu.at[zz, j, m], hrecv.at[zz, j, m], up)

    def h_dn(zz, j, m):
        return rcopy(h_blk(zz, j, m), h_blk(zz, j, m), hsd.at[zz, j, m], hrecv.at[zz, j, m], dn)

    def goes_up(zz):
        return jnp.logical_and(z < 3, jnp.logical_not(jnp.logical_and(z == 2, zz == moved)))

    def goes_dn(zz):
        return jnp.logical_and(z > 0, jnp.logical_not(jnp.logical_and(z == 1, zz == moved)))

    def wx_desc(j, ct):
        return rcopy(w2_ref.at[pl.ds(ct * fhalf + j * nc, nc), :], w2x.at[j], wxs.at[j, ct], wxr.at[j],
                     (dp, z_in, 2 * yy + ct))

    def px_desc(m):
        return rcopy(accx.at[pl.ds(m * hrow + (1 - c) * mbt, mbt), :], partx.at[pl.ds(m * mbt, mbt), :],
                     pxs.at[m], pxr.at[m], partner)

    def pe_desc():
        return rcopy(partx, parte, pes, per, (dp, z_end, row))

    barrier = pltpu.get_barrier_semaphore()
    peers = [partner, xnb] + ynb + zoth + zoth2
    for dev in peers:
        pl.semaphore_signal(barrier, inc=1, device_id=dev, device_id_type=MESH)
    pl.semaphore_wait(barrier, len(peers))

    def own_x_send(m):
        @pl.when(z < 3)
        def _():
            x_up(z, m, x_src(m)).start()

        @pl.when(z > 0)
        def _():
            x_dn(z, m, x_src(m)).start()

        x_part(z, m, x_src(m)).start()

    own_x_send(0)
    own_x = [pltpu.make_async_copy(x_src(m), x_blk(z, m), lsem.at[m]) for m in range(2)]
    own_x[0].start()
    own_x[1].start()
    res_x = pltpu.make_async_copy(x_ref, xres, lsem.at[2])
    res_x.start()
    own_g = pltpu.make_async_copy(gamma_ref, gg.at[z], lsem.at[3])
    own_g.start()
    for k in range(3):
        rcopy(gamma_ref, gg.at[z], gs.at[k], gr.at[z], zoth[k]).start()

    def start_w(w):
        def body(j, _):
            p_desc(w, j).start()
            for ct in range(2):
                y_desc(w, j, ct).start()
            return 0
        lax.fori_loop(0, NCHUNK, body, 0)

    def start_wx(js):
        @pl.when(jnp.logical_and(end, row == moved))
        def _():
            for j in js:
                for ct in range(2):
                    wx_desc(j, ct).start()

    def zero():
        def body(i, _):
            rs = pl.ds(pl.multiple_of(i * 64, 64), 64)
            acc[rs, :] = jnp.zeros((64, acc.shape[1]), jnp.float32)
            accx[rs, :] = jnp.zeros((64, acc.shape[1]), jnp.float32)
            return 0
        lax.fori_loop(0, toks // 64, body, 0)

    def xhop(h, m):
        @pl.when(z >= h)
        def _():
            x_up(z - h, m).wait_recv()

            @pl.when(z < 3)
            def _():
                x_up(z - h, m).start()
            x_part(z - h, m).start()

        @pl.when(z + h <= 3)
        def _():
            x_dn(z + h, m).wait_recv()

            @pl.when(z > 0)
            def _():
                x_dn(z + h, m).start()
            x_part(z + h, m).start()

    def x_done(m):
        for zz in range(4):
            blk = xg.at[zz, pl.ds(m * hrow + (1 - c) * mbt, mbt), :]
            rcopy(blk, blk, xps.at[zz, m], xpr.at[zz, m], partner).wait_recv()
        own_x[m].wait()

    def gamma_done():
        own_g.wait()
        res_x.wait()
        for k in range(3):
            zo = (z + k + 1) % 4
            rcopy(gg.at[zo], gg.at[zo], gs.at[k], gr.at[zo], zoth[k]).wait_recv()

    def norm(m):
        def body(i, _):
            rs = pl.ds(pl.multiple_of(m * hrow + i * LN_ROWS, LN_ROWS), LN_ROWS)
            s1 = jnp.zeros((LN_ROWS, 1), jnp.float32)
            s2 = jnp.zeros((LN_ROWS, 1), jnp.float32)
            for q in range(4):
                v = xg[q, rs, :].astype(jnp.float32)
                s1 += jnp.sum(v, axis=-1, keepdims=True)
                s2 += jnp.sum(v * v, axis=-1, keepdims=True)
            mean = s1 / d_model
            inv = lax.rsqrt(s2 / d_model - mean * mean + LN_EPS)
            for q in range(4):
                v = xg[q, rs, :].astype(jnp.float32)
                g = gg[q, 0:1, :]
                zv[rs, q * dblk:(q + 1) * dblk] = ((v - mean) * inv * g).astype(jnp.bfloat16)
            return 0
        lax.fori_loop(0, hrow // LN_ROWS, body, 0)

    def w1_loads(j, s):
        out = []
        for k in range(4):
            rr = (row + k) % 4
            dst = wbuf.at[s, pl.ds(rr * rows1, rows1), :]
            if k == 0:
                src = w1_ref.at[:, pl.ds(c * fhalf + j * nc + s * nt, nt)]
            else:
                src = w1g.at[j, rr, :, pl.ds(s * nt, nt)]
            out.append(pltpu.make_async_copy(src, dst, wsem.at[s, k]))
        return out

    ntile = nc // nt

    def w1_ready(j):
        p_arrive(0, j)
        x_arrive(0, j)
        for s in range(ntile):
            for cp in w1_loads(j, s):
                cp.start()

    def mat1(j, lo=0, hi=2):
        for m in range(lo, hi):
            def tile(s, _):
                if m == lo and lo == 0:
                    for cp in w1_loads(j, s):
                        cp.wait()
                u = jnp.dot(zv[m * hrow:(m + 1) * hrow, :], wbuf[s], preferred_element_type=jnp.float32)
                hst[m * hrow:(m + 1) * hrow, pl.ds(pl.multiple_of(s * nt, nt), nt)] = jax.nn.gelu(
                    u, approximate=True).astype(jnp.bfloat16)
                return 0
            lax.fori_loop(0, ntile, tile, 0)
            st = pltpu.make_async_copy(hst.at[pl.ds(m * hrow, hrow), :], h_blk(z, j, m), hsem.at[0])
            st.start()
            st.wait()

            @pl.when(goes_up(z))
            def _():
                h_up(z, j, m).start()

            @pl.when(goes_dn(z))
            def _():
                h_dn(z, j, m).start()

    def hop(h, j, ms=(0, 1)):
        for m in ms:
            @pl.when(jnp.logical_and(z >= h, jnp.logical_not(jnp.logical_and(z == 3, z - h == moved))))
            def _():
                h_up(z - h, j, m).wait_recv()

                @pl.when(goes_up(z - h))
                def _():
                    h_up(z - h, j, m).start()

            @pl.when(jnp.logical_and(z + h <= 3, jnp.logical_not(jnp.logical_and(z == 0, z + h == moved))))
            def _():
                h_dn(z + h, j, m).wait_recv()

                @pl.when(goes_dn(z + h))
                def _():
                    h_dn(z + h, j, m).start()

    def mat2(pair, j):
        def load(s, zz):
            dst = w2in.at[s]

            @pl.when(zz == row)
            def _():
                pltpu.make_async_copy(w2_ref.at[pl.ds(c * fhalf + j * nc, nc), :], dst, msem.at[s, 0]).start()

            @pl.when(zz != row)
            def _():
                pltpu.make_async_copy(w2g.at[zz, j], dst, msem.at[s, 0]).start()
            pltpu.make_async_copy(hg.at[zz, j], hin.at[s], msem.at[s, 1]).start()

        def runs(zz):
            return jnp.logical_not(jnp.logical_and(end, zz == moved))

        for s in range(2):
            @pl.when(runs(pair[s]))
            def _():
                load(s, pair[s])

        def block(s, _):
            zz = jnp.where(s == 0, pair[0], pair[1])

            @pl.when(runs(zz))
            def _():
                pltpu.make_async_copy(w2g.at[zz, j], w2in.at[s], msem.at[s, 0]).wait()
                pltpu.make_async_copy(hg.at[zz, j], hin.at[s], msem.at[s, 1]).wait()

                def mtile(m, _):
                    ms = pl.ds(pl.multiple_of(m * 256, 256), 256)
                    acc[ms, :] += jnp.dot(hin[s, ms, :], w2in[s], preferred_element_type=jnp.float32)
                    return 0
                lax.fori_loop(0, toks // 256, mtile, 0)
            return 0
        lax.fori_loop(0, 2, block, 0)

    pair_a = (z, z + 1 - 2 * (z % 2))
    zb = (z + 2) % 4
    pair_b = (zb, zb + 1 - 2 * (zb % 2))

    def w2_ready(j):
        p_arrive(1, j)
        x_arrive(1, j)

    def mat2x(j):
        @pl.when(inner)
        def _():
            rcopy(w2x.at[j], w2x.at[j], wxs.at[j, 0], wxr.at[j], partner).wait_recv()
            a = pltpu.make_async_copy(w2x.at[j], w2in.at[0], msem.at[0, 0])
            b = pltpu.make_async_copy(hg.at[moved, j], hin.at[0], msem.at[0, 1])
            a.start()
            b.start()
            a.wait()
            b.wait()

            def mtile(m, _):
                ms = pl.ds(pl.multiple_of(m * 256, 256), 256)
                accx[ms, :] += jnp.dot(hin[0, ms, :], w2in[0], preferred_element_type=jnp.float32)
                return 0
            lax.fori_loop(0, toks // 256, mtile, 0)

    def px_start():
        @pl.when(inner)
        def _():
            for m in range(2):
                px_desc(m).start()

    def px_finish():
        @pl.when(inner)
        def _():
            for m in range(2):
                px_desc(m).wait_recv()

                def add(i, _):
                    a = pl.ds(pl.multiple_of(m * hrow + c * mbt + i * 64, 64), 64)
                    b = pl.ds(pl.multiple_of(m * mbt + i * 64, 64), 64)
                    partx[b, :] += accx[a, :]
                    return 0
                lax.fori_loop(0, mbt // 64, add, 0)
            pe_desc().start()

    start_w(0)
    zero()
    xhop(1, 0)
    xhop(2, 0)
    own_x_send(1)
    start_wx((0, 1, 2))
    y_arrive_forward(0, 0)
    xhop(3, 0)
    x_done(0)
    gamma_done()
    norm(0)
    xhop(1, 1)
    y_arrive_forward(0, 1)
    xhop(2, 1)
    w1_ready(0)
    mat1(0, 0, 1)
    xhop(3, 1)
    x_done(1)
    norm(1)
    mat1(0, 1, 2)
    y_arrive_forward(0, 2)
    start_w(1)
    w1_ready(1)
    mat1(1)
    hop(1, 0)
    y_arrive_forward(0, 3)
    w1_ready(2)
    mat1(2)
    start_wx((3,))
    hop(1, 1)
    y_arrive_forward(0, 4)
    w1_ready(3)
    mat1(3)
    start_wx((4,))
    hop(2, 0)
    hop(1, 2)
    y_arrive_forward(0, 5)
    w1_ready(4)
    mat1(4)
    start_wx((5,))
    hop(2, 1)
    w1_ready(5)
    mat1(5)
    hop(1, 3)
    y_arrive_forward(1, 0)
    hop(2, 2)
    y_arrive_forward(1, 1)
    hop(1, 4)
    w2_ready(0)
    mat2(pair_a, 0)
    mat2x(0)
    mat2x(1)
    hop(2, 3)
    y_arrive_forward(1, 2)
    w2_ready(1)
    mat2(pair_a, 1)
    mat2x(2)
    mat2x(3)
    hop(1, 5)
    y_arrive_forward(1, 3)
    w2_ready(2)
    mat2(pair_a, 2)
    mat2x(4)
    hop(2, 4)
    mat2x(5)
    px_start()
    hop(2, 5)
    y_arrive_forward(1, 4)
    px_finish()
    w2_ready(3)
    mat2(pair_a, 3)
    hop(3, 0)
    mat2(pair_b, 0)
    y_arrive_forward(1, 5)
    hop(3, 1)
    mat2(pair_b, 1)
    w2_ready(4)
    mat2(pair_a, 4)
    hop(3, 2)
    mat2(pair_b, 2)
    hop(3, 3)
    mat2(pair_b, 3)
    w2_ready(5)
    mat2(pair_a, 5)
    hop(3, 4)
    mat2(pair_b, 4)
    hop(3, 5)
    mat2(pair_b, 5)
    def fin_desc(m):
        return rcopy(acc.at[pl.ds(m * hrow + (1 - c) * mbt, mbt), :], part.at[pl.ds(m * mbt, mbt), :],
                     fs.at[m], fr.at[m], partner)
    for m in range(2):
        fin_desc(m).start()

    @pl.when(end)
    def _():
        pe_desc().wait_recv()

        def add(i, _):
            for m in range(2):
                a = pl.ds(pl.multiple_of(m * hrow + c * mbt + i * 64, 64), 64)
                b = pl.ds(pl.multiple_of(m * mbt + i * 64, 64), 64)
                acc[a, :] += parte[b, :]
            return 0
        lax.fori_loop(0, mbt // 64, add, 0)

    for m in range(2):
        fin_desc(m).wait()

        def final(i, _):
            a = pl.ds(pl.multiple_of(m * hrow + c * mbt + i * 64, 64), 64)
            b = pl.ds(pl.multiple_of(m * mbt + i * 64, 64), 64)
            y_ref[b, :] = (xres[b, :].astype(jnp.float32) + (acc[a, :] + part[b, :])).astype(jnp.bfloat16)
            return 0
        lax.fori_loop(0, mbt // 64, final, 0)

    for w in range(2):
        def drain(j, _):
            p_desc(w, j).wait_send()
            for ct in range(2):
                y_desc(w, j, ct).wait_send()
            x_sent(w, j)
            return 0
        lax.fori_loop(0, NCHUNK, drain, 0)
    for k in range(3):
        rcopy(gamma_ref, gg.at[z], gs.at[k], gr.at[z], zoth[k]).wait_send()

    def drain_z(zz, _):
        for m in range(2):
            x_part(zz, m).wait_send()

        @pl.when(jnp.logical_and(zz <= z, z < 3))
        def _():
            for m in range(2):
                x_up(zz, m).wait_send()

        @pl.when(jnp.logical_and(zz >= z, z > 0))
        def _():
            for m in range(2):
                x_dn(zz, m).wait_send()

        @pl.when(jnp.logical_and(zz <= z, goes_up(zz)))
        def _():
            def d(j, _):
                for m in range(2):
                    h_up(zz, j, m).wait_send()
                return 0
            lax.fori_loop(0, NCHUNK, d, 0)

        @pl.when(jnp.logical_and(zz >= z, goes_dn(zz)))
        def _():
            def d(j, _):
                for m in range(2):
                    h_dn(zz, j, m).wait_send()
                return 0
            lax.fori_loop(0, NCHUNK, d, 0)
        return 0
    lax.fori_loop(0, 4, drain_z, 0)

    @pl.when(jnp.logical_and(end, row == moved))
    def _():
        def d(j, _):
            for ct in range(2):
                wx_desc(j, ct).wait_send()
            return 0
        lax.fori_loop(0, NCHUNK, d, 0)

    @pl.when(inner)
    def _():
        for m in range(2):
            px_desc(m).wait_send()
        pe_desc().wait_send()


def solution(mesh):
    act_spec = P(None, ("dp", "row"), "col")

    def per_device(x_blk, gamma_blk, w_in_blk, w_out_blk):
        mb, rows, dblk = x_blk.shape
        tok = mb * rows
        fz = w_in_blk.shape[1]
        fhalf = fz // 2
        nc = fhalf // NCHUNK
        bf16, f32 = jnp.bfloat16, jnp.float32
        x2 = x_blk.reshape(tok, dblk)
        g2 = jnp.broadcast_to(gamma_blk[None, :], (8, dblk))
        dma = pltpu.SemaphoreType.DMA
        anyspec = pl.BlockSpec(memory_space=pl.ANY)
        out = pl.pallas_call(
            _kernel,
            out_shape=(
                jax.ShapeDtypeStruct((tok, dblk), bf16),
                jax.ShapeDtypeStruct((NCHUNK, 4, w_in_blk.shape[0], nc), bf16),
                jax.ShapeDtypeStruct((4, NCHUNK, nc, dblk), bf16),
                jax.ShapeDtypeStruct((4, NCHUNK, 2 * tok, nc), bf16),
                jax.ShapeDtypeStruct((NCHUNK, nc, dblk), bf16),
            ),
            in_specs=[anyspec] * 4,
            out_specs=(pl.BlockSpec(memory_space=pltpu.VMEM), anyspec, anyspec, anyspec, anyspec),
            scratch_shapes=[
                pltpu.VMEM((4, 2 * tok, dblk), bf16),
                pltpu.VMEM((2 * tok, 4 * dblk), bf16),
                pltpu.VMEM((4, 8, dblk), f32),
                pltpu.VMEM((2, 4 * dblk, 256), bf16),
                pltpu.VMEM((2 * tok, nc), bf16),
                pltpu.VMEM((2 * tok, dblk), f32),
                pltpu.VMEM((2 * tok, dblk), f32),
                pltpu.VMEM((2, 2 * tok, nc), bf16),
                pltpu.VMEM((2, nc, dblk), bf16),
                pltpu.VMEM((tok, dblk), f32),
                pltpu.VMEM((tok, dblk), f32),
                pltpu.VMEM((tok, dblk), f32),
                pltpu.VMEM((tok, dblk), bf16),
                dma((2, NCHUNK, 2)), dma((2, NCHUNK, 2)), dma((2, NCHUNK, 2)), dma((2, NCHUNK, 2)),
                dma((2, NCHUNK)), dma((2, NCHUNK)),
                dma((4, 2)), dma((4, 2)), dma((4, 2)), dma((4, 2)), dma((4, 2)), dma((3,)), dma((4,)),
                dma((4, NCHUNK, 2)), dma((4, NCHUNK, 2)), dma((4, NCHUNK, 2)), dma((2,)), dma((2,)),
                dma((NCHUNK, 2)), dma((NCHUNK,)), dma((2,)), dma((2,)), dma, dma,
                dma((4,)), dma((2, 4)), dma((1,)), dma((2, 2)),
            ],
            compiler_params=pltpu.CompilerParams(
                collective_id=0, has_side_effects=True, vmem_limit_bytes=66_000_000),
            name="mlp",
        )(x2, g2, w_in_blk, w_out_blk)
        return out[0].reshape(mb, rows, dblk)

    return jax.shard_map(
        per_device, mesh=mesh, in_specs=(act_spec, P("col"), P("row", "col"), P("row", "col")),
        out_specs=act_spec, check_vma=False)
```

```python
import functools

import jax
import jax.numpy as jnp
from jax import lax
from jax.experimental import pallas as pl
from jax.experimental.pallas import tpu as pltpu
from jax.sharding import PartitionSpec as P

LN_EPS = 1e-5
MESH = pl.DeviceIdType.MESH
NCHUNK = 6
LN_ROWS = 16
EXTRA = ()
ORDER = (
    "own_1", "wx_1", "g", "y_0_0", "wx_0", "x_1_0", "x_2_0", "w_1", "x_1_1", "x_3_0", "p_0", "y_0_1",
    "xd_0", "ln_0", "x_2_1", "f_0_0_1", "x_3_1", "y_0_2", "xd_1", "ln_1", "f_0_1_2", "p_1", "f_1",
    "h_1_0_0", "y_0_3", "h_1_0_1", "p_2", "h_2_0_0", "f_2", "h_1_1_0", "wx_3", "h_2_0_1", "y_0_4",
    "h_1_2_0", "h_1_1_1", "h_1_2_1", "p_3", "f_3", "y_0_5", "q_4", "q_1", "q_3", "p_4", "h_2_1_0",
    "h_3_0_1", "h_2_2_0", "f_4", "y_1_0", "c_0", "wx_2", "q_0", "h_3_0_0", "q_2", "h_1_3_0", "h_2_1_1",
    "h_1_3_1", "h_3_1_0", "c_1", "h_1_4_0", "p_5", "f_5", "h_1_4_1", "y_1_1", "h_3_1_1", "r_0",
    "h_2_3_1", "h_2_3_0", "wx_4", "a_0", "h_3_2_0", "h_2_2_1", "h_2_4_0", "y_1_2", "h_1_5_1", "wx_5",
    "h_1_5_0", "c_2", "y_1_3", "c_4", "h_3_3_0", "h_3_3_1", "b_0", "h_2_5_1", "r_2", "r_1", "h_3_2_1",
    "c_3", "a_2", "a_1", "h_2_5_0", "b_2", "h_2_4_1", "c_5", "q_5", "r_3", "y_1_4", "h_3_4_0",
    "h_3_4_1", "ps", "pf", "a_3", "y_1_5", "r_4", "b_3", "b_4", "h_3_5_1", "a_4", "b_1", "h_3_5_0",
    "a_5", "r_5", "b_5",
)


def _kernel(
    x_ref, gamma_ref, w1_ref, w2_ref,
    y_ref, w1g, w2g, hg, w2x, w2y,
    xg, zv, gg, wbuf, hst, acc, accx, hin, w2in, part, partx, parte, xres,
    ys, yr, xs, xr, ps, pr,
    xsu, xsd, xrecv, xps, xpr, gs, gr, hsu, hsd, hrecv, fs, fr,
    wxs, wxr, wx2s, wx2r, pxs, pxr, pes, per,
    lsem, wsem, hsem, msem,
):
    dp, z, row = lax.axis_index("dp"), lax.axis_index("col"), lax.axis_index("row")
    yy, c = row // 2, row % 2
    tok, dblk = x_ref.shape
    toks = 2 * tok
    rows1, fz = w1_ref.shape
    fhalf = fz // 2
    nc = fhalf // NCHUNK
    half1, half2 = rows1 // 2, nc // 2
    nt = wbuf.shape[2]
    d_model = 4 * dblk

    partner = (dp, z, 2 * yy + (1 - c))
    xnb = (1 - dp, z, row)
    ynb = [(dp, z, 2 * (1 - yy) + ct) for ct in range(2)]
    up = (dp, jnp.minimum(z + 1, 3), row)
    dn = (dp, jnp.maximum(z - 1, 0), row)
    zoth = [(dp, (z + k) % 4, row) for k in range(1, 4)]
    zoth2 = [(dp, (z + k) % 4, 2 * yy + (1 - c)) for k in range(1, 4)]
    mbt = tok // 2
    hrow = 2 * mbt
    end = jnp.logical_or(z == 0, z == 3)
    inner = jnp.logical_not(end)
    moved = 1 + yy
    z_in = jnp.where(z < 2, 1, 2)
    z_end = jnp.where(z < 2, 0, 3)
    far = 3 - z_end

    def rcopy(src, dst, ssem, rsem, dev):
        return pltpu.make_async_remote_copy(
            src_ref=src, dst_ref=dst, send_sem=ssem, recv_sem=rsem, device_id=dev, device_id_type=MESH)

    def y_desc(w, j, ct):
        if w == 0:
            src = w1_ref.at[pl.ds(dp * half1, half1), pl.ds(ct * fhalf + j * nc, nc)]
            dst = w1g.at[j, row, pl.ds(dp * half1, half1), :]
        else:
            src = w2_ref.at[pl.ds(ct * fhalf + j * nc + dp * half2, half2), :]
            dst = w2g.at[row, j, pl.ds(dp * half2, half2), :]
        return rcopy(src, dst, ys.at[w, j, ct], yr.at[w, j, c], ynb[ct])

    def region(w, j, cs, side):
        rr = 2 * (1 - yy) + cs
        if w == 0:
            return w1g.at[j, rr, pl.ds(side * half1, half1), :]
        return w2g.at[rr, j, pl.ds(side * half2, half2), :]

    def y_arrive_forward(w, j):
        for cs in range(2):
            reg = region(w, j, cs, dp)
            rcopy(reg, reg, ys.at[w, j, cs], yr.at[w, j, cs], ynb[cs]).wait_recv()
            rcopy(reg, reg, xs.at[w, j, cs], xr.at[w, j, cs], xnb).start()

    def x_arrive(w, j):
        for cs in range(2):
            reg = region(w, j, cs, 1 - dp)
            rcopy(reg, reg, xs.at[w, j, cs], xr.at[w, j, cs], xnb).wait_recv()

    def x_sent(w, j):
        for cs in range(2):
            reg = region(w, j, cs, dp)
            rcopy(reg, reg, xs.at[w, j, cs], xr.at[w, j, cs], xnb).wait_send()

    def p_desc(w, j):
        if w == 0:
            src = w1_ref.at[:, pl.ds((1 - c) * fhalf + j * nc, nc)]
            dst = w1g.at[j, row]
        else:
            src = w2_ref.at[pl.ds((1 - c) * fhalf + j * nc, nc), :]
            dst = w2g.at[row, j]
        return rcopy(src, dst, ps.at[w, j], pr.at[w, j], partner)

    def p_arrive(w, j):
        rp = 2 * yy + (1 - c)
        dst = w1g.at[j, rp] if w == 0 else w2g.at[rp, j]
        rcopy(dst, dst, ps.at[w, j], pr.at[w, j], partner).wait_recv()

    def x_blk(zz, m):
        return xg.at[zz, pl.ds(m * hrow + c * mbt, mbt), :]

    def x_src(m):
        return x_ref.at[pl.ds(m * mbt, mbt), :]

    def x_up(zz, m, src=None):
        return rcopy(x_blk(zz, m) if src is None else src, x_blk(zz, m), xsu.at[zz, m], xrecv.at[zz, m], up)

    def x_dn(zz, m, src=None):
        return rcopy(x_blk(zz, m) if src is None else src, x_blk(zz, m), xsd.at[zz, m], xrecv.at[zz, m], dn)

    def x_part(zz, m, src=None):
        return rcopy(x_blk(zz, m) if src is None else src, x_blk(zz, m), xps.at[zz, m], xpr.at[zz, m], partner)

    def h_blk(zz, j, m):
        return hg.at[zz, j, pl.ds(m * hrow, hrow), :]

    def h_up(zz, j, m):
        return rcopy(h_blk(zz, j, m), h_blk(zz, j, m), hsu.at[zz, j, m], hrecv.at[zz, j, m], up)

    def h_dn(zz, j, m):
        return rcopy(h_blk(zz, j, m), h_blk(zz, j, m), hsd.at[zz, j, m], hrecv.at[zz, j, m], dn)

    def not_taken(e, zz, j):
        if j in EXTRA:
            return jnp.logical_or(zz == moved, zz == 3 - e)
        return zz == moved

    def goes_up(zz, j):
        return jnp.logical_and(z < 3, jnp.logical_not(jnp.logical_and(z == 2, not_taken(3, zz, j))))

    def goes_dn(zz, j):
        return jnp.logical_and(z > 0, jnp.logical_not(jnp.logical_and(z == 1, not_taken(0, zz, j))))

    def wx_desc(j, ct):
        return rcopy(w2_ref.at[pl.ds(ct * fhalf + j * nc, nc), :], w2x.at[j], wxs.at[j, ct], wxr.at[j],
                     (dp, z_in, 2 * yy + ct))

    def wx2_desc(j, own):
        src = w2_ref.at[pl.ds(c * fhalf + j * nc, nc), :] if own else w2g.at[far, j]
        return rcopy(src, w2y.at[EXTRA.index(j)], wx2s.at[EXTRA.index(j)], wx2r.at[EXTRA.index(j)], (dp, z_in, row))

    def px_desc(m):
        return rcopy(accx.at[pl.ds(m * hrow + (1 - c) * mbt, mbt), :], partx.at[pl.ds(m * mbt, mbt), :],
                     pxs.at[m], pxr.at[m], partner)

    def pe_desc():
        return rcopy(partx, parte, pes, per, (dp, z_end, row))

    barrier = pltpu.get_barrier_semaphore()
    peers = [partner, xnb] + ynb + zoth + zoth2
    for dev in peers:
        pl.semaphore_signal(barrier, inc=1, device_id=dev, device_id_type=MESH)
    pl.semaphore_wait(barrier, len(peers))

    def own_x_send(m):
        @pl.when(z < 3)
        def _():
            x_up(z, m, x_src(m)).start()

        @pl.when(z > 0)
        def _():
            x_dn(z, m, x_src(m)).start()

        x_part(z, m, x_src(m)).start()

    own_x_send(0)
    own_x = [pltpu.make_async_copy(x_src(m), x_blk(z, m), lsem.at[m]) for m in range(2)]
    own_x[0].start()
    own_x[1].start()
    res_x = pltpu.make_async_copy(x_ref, xres, lsem.at[2])
    res_x.start()
    own_g = pltpu.make_async_copy(gamma_ref, gg.at[z], lsem.at[3])
    own_g.start()
    for k in range(3):
        rcopy(gamma_ref, gg.at[z], gs.at[k], gr.at[z], zoth[k]).start()

    def start_w(w):
        def body(j, _):
            p_desc(w, j).start()
            for ct in range(2):
                y_desc(w, j, ct).start()
            return 0
        lax.fori_loop(0, NCHUNK, body, 0)

    def start_wx(js):
        @pl.when(jnp.logical_and(end, row == moved))
        def _():
            for j in js:
                for ct in range(2):
                    wx_desc(j, ct).start()

    def zero():
        def body(i, _):
            rs = pl.ds(pl.multiple_of(i * 64, 64), 64)
            acc[rs, :] = jnp.zeros((64, acc.shape[1]), jnp.float32)
            accx[rs, :] = jnp.zeros((64, acc.shape[1]), jnp.float32)
            return 0
        lax.fori_loop(0, toks // 64, body, 0)

    def xhop(h, m):
        @pl.when(z >= h)
        def _():
            x_up(z - h, m).wait_recv()

            @pl.when(z < 3)
            def _():
                x_up(z - h, m).start()
            x_part(z - h, m).start()

        @pl.when(z + h <= 3)
        def _():
            x_dn(z + h, m).wait_recv()

            @pl.when(z > 0)
            def _():
                x_dn(z + h, m).start()
            x_part(z + h, m).start()

    def x_done(m):
        for zz in range(4):
            blk = xg.at[zz, pl.ds(m * hrow + (1 - c) * mbt, mbt), :]
            rcopy(blk, blk, xps.at[zz, m], xpr.at[zz, m], partner).wait_recv()
        own_x[m].wait()

    def gamma_done():
        own_g.wait()
        res_x.wait()
        for k in range(3):
            zo = (z + k + 1) % 4
            rcopy(gg.at[zo], gg.at[zo], gs.at[k], gr.at[zo], zoth[k]).wait_recv()

    def norm(m):
        def body(i, _):
            rs = pl.ds(pl.multiple_of(m * hrow + i * LN_ROWS, LN_ROWS), LN_ROWS)
            s1 = jnp.zeros((LN_ROWS, 1), jnp.float32)
            s2 = jnp.zeros((LN_ROWS, 1), jnp.float32)
            for q in range(4):
                v = xg[q, rs, :].astype(jnp.float32)
                s1 += jnp.sum(v, axis=-1, keepdims=True)
                s2 += jnp.sum(v * v, axis=-1, keepdims=True)
            mean = s1 / d_model
            inv = lax.rsqrt(s2 / d_model - mean * mean + LN_EPS)
            for q in range(4):
                v = xg[q, rs, :].astype(jnp.float32)
                g = gg[q, 0:1, :]
                zv[rs, q * dblk:(q + 1) * dblk] = ((v - mean) * inv * g).astype(jnp.bfloat16)
            return 0
        lax.fori_loop(0, hrow // LN_ROWS, body, 0)

    def w1_loads(j, s):
        out = []
        for k in range(4):
            rr = (row + k) % 4
            dst = wbuf.at[s, pl.ds(rr * rows1, rows1), :]
            if k == 0:
                src = w1_ref.at[:, pl.ds(c * fhalf + j * nc + s * nt, nt)]
            else:
                src = w1g.at[j, rr, :, pl.ds(s * nt, nt)]
            out.append(pltpu.make_async_copy(src, dst, wsem.at[s, k]))
        return out

    ntile = nc // nt

    def w1_ready(j):
        p_arrive(0, j)
        x_arrive(0, j)
        for s in range(ntile):
            for cp in w1_loads(j, s):
                cp.start()

    def mat1(j, lo=0, hi=2):
        for m in range(lo, hi):
            def tile(s, _):
                if m == lo and lo == 0:
                    for cp in w1_loads(j, s):
                        cp.wait()
                u = jnp.dot(zv[m * hrow:(m + 1) * hrow, :], wbuf[s], preferred_element_type=jnp.float32)
                hst[m * hrow:(m + 1) * hrow, pl.ds(pl.multiple_of(s * nt, nt), nt)] = jax.nn.gelu(
                    u, approximate=True).astype(jnp.bfloat16)
                return 0
            lax.fori_loop(0, ntile, tile, 0)
            st = pltpu.make_async_copy(hst.at[pl.ds(m * hrow, hrow), :], h_blk(z, j, m), hsem.at[0])
            st.start()
            st.wait()

            @pl.when(goes_up(z, j))
            def _():
                h_up(z, j, m).start()

            @pl.when(goes_dn(z, j))
            def _():
                h_dn(z, j, m).start()

    def hop(h, j, *ms):
        for m in ms:
            @pl.when(jnp.logical_and(z >= h, jnp.logical_not(jnp.logical_and(z == 3, not_taken(3, z - h, j)))))
            def _():
                h_up(z - h, j, m).wait_recv()

                @pl.when(goes_up(z - h, j))
                def _():
                    h_up(z - h, j, m).start()

            @pl.when(jnp.logical_and(z + h <= 3, jnp.logical_not(jnp.logical_and(z == 0, not_taken(0, z + h, j)))))
            def _():
                h_dn(z + h, j, m).wait_recv()

                @pl.when(goes_dn(z + h, j))
                def _():
                    h_dn(z + h, j, m).start()

    def mat2(pair, j):
        def load(s, zz):
            dst = w2in.at[s]

            @pl.when(zz == row)
            def _():
                pltpu.make_async_copy(w2_ref.at[pl.ds(c * fhalf + j * nc, nc), :], dst, msem.at[s, 0]).start()

            @pl.when(zz != row)
            def _():
                pltpu.make_async_copy(w2g.at[zz, j], dst, msem.at[s, 0]).start()
            pltpu.make_async_copy(hg.at[zz, j], hin.at[s], msem.at[s, 1]).start()

        def runs(zz):
            return jnp.logical_not(jnp.logical_and(end, not_taken(z_end, zz, j)))

        for s in range(2):
            @pl.when(runs(pair[s]))
            def _():
                load(s, pair[s])

        def block(s, _):
            zz = jnp.where(s == 0, pair[0], pair[1])

            @pl.when(runs(zz))
            def _():
                pltpu.make_async_copy(w2g.at[zz, j], w2in.at[s], msem.at[s, 0]).wait()
                pltpu.make_async_copy(hg.at[zz, j], hin.at[s], msem.at[s, 1]).wait()

                def mtile(m, _):
                    ms = pl.ds(pl.multiple_of(m * 256, 256), 256)
                    acc[ms, :] += jnp.dot(hin[s, ms, :], w2in[s], preferred_element_type=jnp.float32)
                    return 0
                lax.fori_loop(0, toks // 256, mtile, 0)
            return 0
        lax.fori_loop(0, 2, block, 0)

    pair_a = (2 * yy, 2 * yy + 1)
    pair_b = (2 - 2 * yy, 3 - 2 * yy)

    def w2_local(j):
        p_arrive(1, j)

    def w2_remote(j):
        x_arrive(1, j)

    def mat2x(j):
        @pl.when(inner)
        def _():
            rcopy(w2x.at[j], w2x.at[j], wxs.at[j, 0], wxr.at[j], partner).wait_recv()
            a = pltpu.make_async_copy(w2x.at[j], w2in.at[0], msem.at[0, 0])
            b = pltpu.make_async_copy(hg.at[moved, j], hin.at[0], msem.at[0, 1])
            a.start()
            b.start()
            a.wait()
            b.wait()

            def mtile(m, _):
                ms = pl.ds(pl.multiple_of(m * 256, 256), 256)
                accx[ms, :] += jnp.dot(hin[0, ms, :], w2in[0], preferred_element_type=jnp.float32)
                return 0
            lax.fori_loop(0, toks // 256, mtile, 0)

    def start_wx2(j):
        @pl.when(jnp.logical_and(end, row == far))
        def _():
            wx2_desc(j, True).start()

        @pl.when(jnp.logical_and(end, row != far))
        def _():
            wx2_desc(j, False).start()

    def mat2y(j):
        i = EXTRA.index(j)

        @pl.when(inner)
        def _():
            rcopy(w2y.at[i], w2y.at[i], wx2s.at[i], wx2r.at[i], partner).wait_recv()
            a = pltpu.make_async_copy(w2y.at[i], w2in.at[0], msem.at[0, 0])
            b = pltpu.make_async_copy(hg.at[far, j], hin.at[0], msem.at[0, 1])
            a.start()
            b.start()
            a.wait()
            b.wait()

            def mtile(m, _):
                ms = pl.ds(pl.multiple_of(m * 256, 256), 256)
                accx[ms, :] += jnp.dot(hin[0, ms, :], w2in[0], preferred_element_type=jnp.float32)
                return 0
            lax.fori_loop(0, toks // 256, mtile, 0)

    def px_start():
        @pl.when(inner)
        def _():
            for m in range(2):
                px_desc(m).start()

    def px_finish():
        @pl.when(inner)
        def _():
            for m in range(2):
                px_desc(m).wait_recv()

                def add(i, _):
                    a = pl.ds(pl.multiple_of(m * hrow + c * mbt + i * 64, 64), 64)
                    b = pl.ds(pl.multiple_of(m * mbt + i * 64, 64), 64)
                    partx[b, :] += accx[a, :]
                    return 0
                lax.fori_loop(0, mbt // 64, add, 0)
            pe_desc().start()

    start_w(0)
    zero()
    events = dict(
        own=own_x_send, x=xhop, xd=x_done, g=gamma_done, ln=norm, y=y_arrive_forward, w=start_w,
        wx=lambda j: start_wx((j,)), wy=start_wx2, p=w1_ready, q=w2_local, r=w2_remote, f=mat1, h=hop,
        a=functools.partial(mat2, pair_a), b=functools.partial(mat2, pair_b), c=mat2x, d=mat2y,
        ps=px_start, pf=px_finish)
    for code in ORDER:
        name, *index = code.split("_")
        events[name](*map(int, index))
    def fin_desc(m):
        return rcopy(acc.at[pl.ds(m * hrow + (1 - c) * mbt, mbt), :], part.at[pl.ds(m * mbt, mbt), :],
                     fs.at[m], fr.at[m], partner)
    for m in range(2):
        fin_desc(m).start()

    @pl.when(end)
    def _():
        pe_desc().wait_recv()

        def add(i, _):
            for m in range(2):
                a = pl.ds(pl.multiple_of(m * hrow + c * mbt + i * 64, 64), 64)
                b = pl.ds(pl.multiple_of(m * mbt + i * 64, 64), 64)
                acc[a, :] += parte[b, :]
            return 0
        lax.fori_loop(0, mbt // 64, add, 0)

    for m in range(2):
        fin_desc(m).wait()

        def final(i, _):
            a = pl.ds(pl.multiple_of(m * hrow + c * mbt + i * 64, 64), 64)
            b = pl.ds(pl.multiple_of(m * mbt + i * 64, 64), 64)
            y_ref[b, :] = (xres[b, :].astype(jnp.float32) + (acc[a, :] + part[b, :])).astype(jnp.bfloat16)
            return 0
        lax.fori_loop(0, mbt // 64, final, 0)

    for w in range(2):
        def drain(j, _):
            p_desc(w, j).wait_send()
            for ct in range(2):
                y_desc(w, j, ct).wait_send()
            x_sent(w, j)
            return 0
        lax.fori_loop(0, NCHUNK, drain, 0)
    for k in range(3):
        rcopy(gamma_ref, gg.at[z], gs.at[k], gr.at[z], zoth[k]).wait_send()

    def drain_z(zz, _):
        for m in range(2):
            x_part(zz, m).wait_send()

        @pl.when(jnp.logical_and(zz <= z, z < 3))
        def _():
            for m in range(2):
                x_up(zz, m).wait_send()

        @pl.when(jnp.logical_and(zz >= z, z > 0))
        def _():
            for m in range(2):
                x_dn(zz, m).wait_send()

        for j in range(NCHUNK):
            @pl.when(jnp.logical_and(zz <= z, goes_up(zz, j)))
            def _():
                for m in range(2):
                    h_up(zz, j, m).wait_send()

            @pl.when(jnp.logical_and(zz >= z, goes_dn(zz, j)))
            def _():
                for m in range(2):
                    h_dn(zz, j, m).wait_send()
        return 0
    lax.fori_loop(0, 4, drain_z, 0)

    @pl.when(jnp.logical_and(end, row == moved))
    def _():
        def d(j, _):
            for ct in range(2):
                wx_desc(j, ct).wait_send()
            return 0
        lax.fori_loop(0, NCHUNK, d, 0)

    @pl.when(end)
    def _():
        for j in EXTRA:
            wx2_desc(j, False).wait_send()

    @pl.when(inner)
    def _():
        for m in range(2):
            px_desc(m).wait_send()
        pe_desc().wait_send()


def solution(mesh):
    act_spec = P(None, ("dp", "row"), "col")

    def per_device(x_blk, gamma_blk, w_in_blk, w_out_blk):
        mb, rows, dblk = x_blk.shape
        tok = mb * rows
        fz = w_in_blk.shape[1]
        fhalf = fz // 2
        nc = fhalf // NCHUNK
        bf16, f32 = jnp.bfloat16, jnp.float32
        x2 = x_blk.reshape(tok, dblk)
        g2 = jnp.broadcast_to(gamma_blk[None, :], (8, dblk))
        dma = pltpu.SemaphoreType.DMA
        anyspec = pl.BlockSpec(memory_space=pl.ANY)
        out = pl.pallas_call(
            _kernel,
            out_shape=(
                jax.ShapeDtypeStruct((tok, dblk), bf16),
                jax.ShapeDtypeStruct((NCHUNK, 4, w_in_blk.shape[0], nc), bf16),
                jax.ShapeDtypeStruct((4, NCHUNK, nc, dblk), bf16),
                jax.ShapeDtypeStruct((4, NCHUNK, 2 * tok, nc), bf16),
                jax.ShapeDtypeStruct((NCHUNK, nc, dblk), bf16),
                jax.ShapeDtypeStruct((max(len(EXTRA), 1), nc, dblk), bf16),
            ),
            in_specs=[anyspec] * 4,
            out_specs=(pl.BlockSpec(memory_space=pltpu.VMEM), anyspec, anyspec, anyspec, anyspec, anyspec),
            scratch_shapes=[
                pltpu.VMEM((4, 2 * tok, dblk), bf16),
                pltpu.VMEM((2 * tok, 4 * dblk), bf16),
                pltpu.VMEM((4, 8, dblk), f32),
                pltpu.VMEM((2, 4 * dblk, 256), bf16),
                pltpu.VMEM((2 * tok, nc), bf16),
                pltpu.VMEM((2 * tok, dblk), f32),
                pltpu.VMEM((2 * tok, dblk), f32),
                pltpu.VMEM((2, 2 * tok, nc), bf16),
                pltpu.VMEM((2, nc, dblk), bf16),
                pltpu.VMEM((tok, dblk), f32),
                pltpu.VMEM((tok, dblk), f32),
                pltpu.VMEM((tok, dblk), f32),
                pltpu.VMEM((tok, dblk), bf16),
                dma((2, NCHUNK, 2)), dma((2, NCHUNK, 2)), dma((2, NCHUNK, 2)), dma((2, NCHUNK, 2)),
                dma((2, NCHUNK)), dma((2, NCHUNK)),
                dma((4, 2)), dma((4, 2)), dma((4, 2)), dma((4, 2)), dma((4, 2)), dma((3,)), dma((4,)),
                dma((4, NCHUNK, 2)), dma((4, NCHUNK, 2)), dma((4, NCHUNK, 2)), dma((2,)), dma((2,)),
                dma((NCHUNK, 2)), dma((NCHUNK,)), dma((max(len(EXTRA), 1),)), dma((max(len(EXTRA), 1),)),
                dma((2,)), dma((2,)), dma, dma,
                dma((4,)), dma((2, 4)), dma((1,)), dma((2, 2)),
            ],
            compiler_params=pltpu.CompilerParams(
                collective_id=0, has_side_effects=True, vmem_limit_bytes=66_000_000),
            name="mlp",
        )(x2, g2, w_in_blk, w_out_blk)
        return out[0].reshape(mb, rows, dblk)

    return jax.shard_map(
        per_device, mesh=mesh, in_specs=(act_spec, P("col"), P("row", "col"), P("row", "col")),
        out_specs=act_spec, check_vma=False)
```

```python
import functools

import jax
import jax.numpy as jnp
from jax import lax
from jax.experimental import pallas as pl
from jax.experimental.pallas import tpu as pltpu
from jax.sharding import PartitionSpec as P

LN_EPS = 1e-5
MESH = pl.DeviceIdType.MESH
NCHUNK = 6
LN_ROWS = 16
EXTRA = ()
ORDER = (
    "own_1", "wx_1", "y_0_0", "x_1_0", "x_2_0", "wx_0", "x_1_1", "y_0_1", "x_3_0", "g", "xd_0", "ln_0",
    "x_2_1", "p_0", "f_0_0_1", "y_0_2", "x_3_1", "xd_1", "ln_1", "f_0_1_2", "w_1", "p_1", "f_1",
    "h_1_0_0", "h_1_0_1", "p_2", "y_0_3", "h_1_1_0", "c_0", "e_0_0", "e_0_1", "f_2", "e_1_0", "h_2_0_0",
    "h_1_1_1", "y_0_4", "e_1_1", "h_1_2_0", "q_3", "h_2_0_1", "e_2_0", "wx_3", "q_2", "h_2_1_0",
    "e_2_1", "p_3", "h_1_2_1", "y_0_5", "f_3", "p_4", "f_4", "h_2_1_1", "h_3_1_0", "h_2_2_0", "e_3_0",
    "h_2_2_1", "e_3_1", "y_1_0", "wx_2", "h_1_3_1", "h_1_3_0", "h_3_0_1", "p_5", "y_1_1", "h_1_4_1",
    "h_1_4_0", "e_4_0", "f_5", "h_3_1_1", "h_2_3_0", "e_4_1", "r_0", "y_1_2", "h_3_0_0", "wx_4", "c_2",
    "h_2_4_0", "r_1", "h_2_3_1", "b_1", "wx_5", "q_0", "c_3", "c_1", "h_3_2_1", "h_3_2_0", "a_2",
    "e_5_1", "e_5_0", "b_0", "h_1_5_1", "h_3_3_0", "r_2", "y_1_3", "h_1_5_0", "a_0", "q_1", "h_3_3_1",
    "h_2_4_1", "c_4", "h_2_5_1", "a_1", "q_4", "a_3", "h_2_5_0", "b_2", "y_1_4", "c_5", "q_5",
    "h_3_4_1", "ps", "r_3", "h_3_5_1", "pf", "h_3_4_0", "h_3_5_0", "b_3", "r_4", "y_1_5", "b_4", "a_5",
    "a_4", "r_5", "b_5",
)


def _kernel(
    x_ref, gamma_ref, w1_ref, w2_ref,
    y_ref, w1g, w2g, hg, w2x, w2y,
    xg, zv, gg, wbuf, hst, acc, accx, hin, w2in, part, partx, parte, xres,
    ys, yr, xs, xr, ps, pr,
    xsu, xsd, xrecv, xps, xpr, gs, gr, hsu, hsd, hrecv, fs, fr,
    wxs, wxr, wx2s, wx2r, pxs, pxr, pes, per,
    lsem, wsem, hsem, msem,
):
    dp, z, row = lax.axis_index("dp"), lax.axis_index("col"), lax.axis_index("row")
    yy, c = row // 2, row % 2
    tok, dblk = x_ref.shape
    toks = 2 * tok
    rows1, fz = w1_ref.shape
    fhalf = fz // 2
    nc = fhalf // NCHUNK
    half1, half2 = rows1 // 2, nc // 2
    nt = wbuf.shape[2]
    d_model = 4 * dblk

    partner = (dp, z, 2 * yy + (1 - c))
    xnb = (1 - dp, z, row)
    ynb = [(dp, z, 2 * (1 - yy) + ct) for ct in range(2)]
    up = (dp, jnp.minimum(z + 1, 3), row)
    dn = (dp, jnp.maximum(z - 1, 0), row)
    zoth = [(dp, (z + k) % 4, row) for k in range(1, 4)]
    zoth2 = [(dp, (z + k) % 4, 2 * yy + (1 - c)) for k in range(1, 4)]
    mbt = tok // 2
    hrow = 2 * mbt
    end = jnp.logical_or(z == 0, z == 3)
    inner = jnp.logical_not(end)
    moved = 1 + yy
    z_in = jnp.where(z < 2, 1, 2)
    z_end = jnp.where(z < 2, 0, 3)
    far = 3 - z_end

    def rcopy(src, dst, ssem, rsem, dev):
        return pltpu.make_async_remote_copy(
            src_ref=src, dst_ref=dst, send_sem=ssem, recv_sem=rsem, device_id=dev, device_id_type=MESH)

    def y_desc(w, j, ct):
        if w == 0:
            src = w1_ref.at[pl.ds(dp * half1, half1), pl.ds(ct * fhalf + j * nc, nc)]
            dst = w1g.at[j, row, pl.ds(dp * half1, half1), :]
        else:
            src = w2_ref.at[pl.ds(ct * fhalf + j * nc + dp * half2, half2), :]
            dst = w2g.at[row, j, pl.ds(dp * half2, half2), :]
        return rcopy(src, dst, ys.at[w, j, ct], yr.at[w, j, c], ynb[ct])

    def region(w, j, cs, side):
        rr = 2 * (1 - yy) + cs
        if w == 0:
            return w1g.at[j, rr, pl.ds(side * half1, half1), :]
        return w2g.at[rr, j, pl.ds(side * half2, half2), :]

    def y_arrive_forward(w, j):
        for cs in range(2):
            reg = region(w, j, cs, dp)
            rcopy(reg, reg, ys.at[w, j, cs], yr.at[w, j, cs], ynb[cs]).wait_recv()
            rcopy(reg, reg, xs.at[w, j, cs], xr.at[w, j, cs], xnb).start()

    def x_arrive(w, j):
        for cs in range(2):
            reg = region(w, j, cs, 1 - dp)
            rcopy(reg, reg, xs.at[w, j, cs], xr.at[w, j, cs], xnb).wait_recv()

    def x_sent(w, j):
        for cs in range(2):
            reg = region(w, j, cs, dp)
            rcopy(reg, reg, xs.at[w, j, cs], xr.at[w, j, cs], xnb).wait_send()

    def p_desc(w, j):
        if w == 0:
            src = w1_ref.at[:, pl.ds((1 - c) * fhalf + j * nc, nc)]
            dst = w1g.at[j, row]
        else:
            src = w2_ref.at[pl.ds((1 - c) * fhalf + j * nc, nc), :]
            dst = w2g.at[row, j]
        return rcopy(src, dst, ps.at[w, j], pr.at[w, j], partner)

    def p_arrive(w, j):
        rp = 2 * yy + (1 - c)
        dst = w1g.at[j, rp] if w == 0 else w2g.at[rp, j]
        rcopy(dst, dst, ps.at[w, j], pr.at[w, j], partner).wait_recv()

    def x_blk(zz, m):
        return xg.at[zz, pl.ds(m * hrow + c * mbt, mbt), :]

    def x_src(m):
        return x_ref.at[pl.ds(m * mbt, mbt), :]

    def x_up(zz, m, src=None):
        return rcopy(x_blk(zz, m) if src is None else src, x_blk(zz, m), xsu.at[zz, m], xrecv.at[zz, m], up)

    def x_dn(zz, m, src=None):
        return rcopy(x_blk(zz, m) if src is None else src, x_blk(zz, m), xsd.at[zz, m], xrecv.at[zz, m], dn)

    def x_part(zz, m, src=None):
        return rcopy(x_blk(zz, m) if src is None else src, x_blk(zz, m), xps.at[zz, m], xpr.at[zz, m], partner)

    def h_blk(zz, j, m):
        return hg.at[zz, j, pl.ds(m * hrow, hrow), :]

    def h_up(zz, j, m):
        return rcopy(h_blk(zz, j, m), h_blk(zz, j, m), hsu.at[zz, j, m], hrecv.at[zz, j, m], up)

    def h_dn(zz, j, m):
        return rcopy(h_blk(zz, j, m), h_blk(zz, j, m), hsd.at[zz, j, m], hrecv.at[zz, j, m], dn)

    def not_taken(e, zz, j):
        if j in EXTRA:
            return jnp.logical_or(zz == moved, zz == 3 - e)
        return zz == moved

    def goes_up(zz, j):
        return jnp.logical_and(z < 3, jnp.logical_not(jnp.logical_and(z == 2, not_taken(3, zz, j))))

    def goes_dn(zz, j):
        return jnp.logical_and(z > 0, jnp.logical_not(jnp.logical_and(z == 1, not_taken(0, zz, j))))

    def wx_desc(j, ct):
        return rcopy(w2_ref.at[pl.ds(ct * fhalf + j * nc, nc), :], w2x.at[j], wxs.at[j, ct], wxr.at[j],
                     (dp, z_in, 2 * yy + ct))

    def wx2_desc(j, own):
        src = w2_ref.at[pl.ds(c * fhalf + j * nc, nc), :] if own else w2g.at[far, j]
        return rcopy(src, w2y.at[EXTRA.index(j)], wx2s.at[EXTRA.index(j)], wx2r.at[EXTRA.index(j)], (dp, z_in, row))

    def px_desc(m):
        return rcopy(accx.at[pl.ds(m * hrow + (1 - c) * mbt, mbt), :], partx.at[pl.ds(m * mbt, mbt), :],
                     pxs.at[m], pxr.at[m], partner)

    def pe_desc():
        return rcopy(partx, parte, pes, per, (dp, z_end, row))

    barrier = pltpu.get_barrier_semaphore()
    peers = [partner, xnb] + ynb + zoth + zoth2
    for dev in peers:
        pl.semaphore_signal(barrier, inc=1, device_id=dev, device_id_type=MESH)
    pl.semaphore_wait(barrier, len(peers))

    def own_x_send(m):
        @pl.when(z < 3)
        def _():
            x_up(z, m, x_src(m)).start()

        @pl.when(z > 0)
        def _():
            x_dn(z, m, x_src(m)).start()

        x_part(z, m, x_src(m)).start()

    own_x_send(0)
    own_x = [pltpu.make_async_copy(x_src(m), x_blk(z, m), lsem.at[m]) for m in range(2)]
    own_x[0].start()
    own_x[1].start()
    res_x = pltpu.make_async_copy(x_ref, xres, lsem.at[2])
    res_x.start()
    own_g = pltpu.make_async_copy(gamma_ref, gg.at[z], lsem.at[3])
    own_g.start()
    for k in range(3):
        rcopy(gamma_ref, gg.at[z], gs.at[k], gr.at[z], zoth[k]).start()

    def start_w(w):
        def body(j, _):
            p_desc(w, j).start()
            for ct in range(2):
                y_desc(w, j, ct).start()
            return 0
        lax.fori_loop(0, NCHUNK, body, 0)

    def start_wx(js):
        @pl.when(jnp.logical_and(end, row == moved))
        def _():
            for j in js:
                for ct in range(2):
                    wx_desc(j, ct).start()

    def zero():
        def body(i, _):
            rs = pl.ds(pl.multiple_of(i * 64, 64), 64)
            acc[rs, :] = jnp.zeros((64, acc.shape[1]), jnp.float32)
            accx[rs, :] = jnp.zeros((64, acc.shape[1]), jnp.float32)
            return 0
        lax.fori_loop(0, toks // 64, body, 0)

    def xhop(h, m):
        @pl.when(z >= h)
        def _():
            x_up(z - h, m).wait_recv()

            @pl.when(z < 3)
            def _():
                x_up(z - h, m).start()
            x_part(z - h, m).start()

        @pl.when(z + h <= 3)
        def _():
            x_dn(z + h, m).wait_recv()

            @pl.when(z > 0)
            def _():
                x_dn(z + h, m).start()
            x_part(z + h, m).start()

    def x_done(m):
        for zz in range(4):
            blk = xg.at[zz, pl.ds(m * hrow + (1 - c) * mbt, mbt), :]
            rcopy(blk, blk, xps.at[zz, m], xpr.at[zz, m], partner).wait_recv()
        own_x[m].wait()

    def gamma_done():
        own_g.wait()
        res_x.wait()
        for k in range(3):
            zo = (z + k + 1) % 4
            rcopy(gg.at[zo], gg.at[zo], gs.at[k], gr.at[zo], zoth[k]).wait_recv()

    def norm(m):
        def body(i, _):
            rs = pl.ds(pl.multiple_of(m * hrow + i * LN_ROWS, LN_ROWS), LN_ROWS)
            s1 = jnp.zeros((LN_ROWS, 1), jnp.float32)
            s2 = jnp.zeros((LN_ROWS, 1), jnp.float32)
            for q in range(4):
                v = xg[q, rs, :].astype(jnp.float32)
                s1 += jnp.sum(v, axis=-1, keepdims=True)
                s2 += jnp.sum(v * v, axis=-1, keepdims=True)
            mean = s1 / d_model
            inv = lax.rsqrt(s2 / d_model - mean * mean + LN_EPS)
            for q in range(4):
                v = xg[q, rs, :].astype(jnp.float32)
                g = gg[q, 0:1, :]
                zv[rs, q * dblk:(q + 1) * dblk] = ((v - mean) * inv * g).astype(jnp.bfloat16)
            return 0
        lax.fori_loop(0, hrow // LN_ROWS, body, 0)

    def w1_loads(j, s):
        out = []
        for k in range(4):
            rr = (row + k) % 4
            dst = wbuf.at[s, pl.ds(rr * rows1, rows1), :]
            if k == 0:
                src = w1_ref.at[:, pl.ds(c * fhalf + j * nc + s * nt, nt)]
            else:
                src = w1g.at[j, rr, :, pl.ds(s * nt, nt)]
            out.append(pltpu.make_async_copy(src, dst, wsem.at[s, k]))
        return out

    ntile = nc // nt

    def w1_ready(j):
        p_arrive(0, j)
        x_arrive(0, j)
        for s in range(ntile):
            for cp in w1_loads(j, s):
                cp.start()

    def mat1(j, lo=0, hi=2):
        for m in range(lo, hi):
            def tile(s, _):
                if m == lo and lo == 0:
                    for cp in w1_loads(j, s):
                        cp.wait()
                u = jnp.dot(zv[m * hrow:(m + 1) * hrow, :], wbuf[s], preferred_element_type=jnp.float32)
                hst[m * hrow:(m + 1) * hrow, pl.ds(pl.multiple_of(s * nt, nt), nt)] = jax.nn.gelu(
                    u, approximate=True).astype(jnp.bfloat16)
                return 0
            lax.fori_loop(0, ntile, tile, 0)
            st = pltpu.make_async_copy(hst.at[pl.ds(m * hrow, hrow), :], h_blk(z, j, m), hsem.at[0])
            st.start()
            st.wait()

            @pl.when(goes_up(z, j))
            def _():
                h_up(z, j, m).start()

            @pl.when(goes_dn(z, j))
            def _():
                h_dn(z, j, m).start()

    def hop(h, j, *ms, from_end=False):
        first = h == 1
        for m in ms:
            @pl.when(jnp.logical_and(jnp.logical_and(z >= h, ((z == 1) == from_end) if first else True), jnp.logical_not(jnp.logical_and(z == 3, not_taken(3, z - h, j)))))
            def _():
                h_up(z - h, j, m).wait_recv()

                @pl.when(goes_up(z - h, j))
                def _():
                    h_up(z - h, j, m).start()

            @pl.when(jnp.logical_and(jnp.logical_and(z + h <= 3, ((z == 2) == from_end) if first else True), jnp.logical_not(jnp.logical_and(z == 0, not_taken(0, z + h, j)))))
            def _():
                h_dn(z + h, j, m).wait_recv()

                @pl.when(goes_dn(z + h, j))
                def _():
                    h_dn(z + h, j, m).start()

    def mat2(pair, j):
        def load(s, zz):
            dst = w2in.at[s]

            @pl.when(zz == row)
            def _():
                pltpu.make_async_copy(w2_ref.at[pl.ds(c * fhalf + j * nc, nc), :], dst, msem.at[s, 0]).start()

            @pl.when(zz != row)
            def _():
                pltpu.make_async_copy(w2g.at[zz, j], dst, msem.at[s, 0]).start()
            pltpu.make_async_copy(hg.at[zz, j], hin.at[s], msem.at[s, 1]).start()

        def runs(zz):
            return jnp.logical_not(jnp.logical_and(end, not_taken(z_end, zz, j)))

        for s in range(2):
            @pl.when(runs(pair[s]))
            def _():
                load(s, pair[s])

        def block(s, _):
            zz = jnp.where(s == 0, pair[0], pair[1])

            @pl.when(runs(zz))
            def _():
                pltpu.make_async_copy(w2g.at[zz, j], w2in.at[s], msem.at[s, 0]).wait()
                pltpu.make_async_copy(hg.at[zz, j], hin.at[s], msem.at[s, 1]).wait()

                def mtile(m, _):
                    ms = pl.ds(pl.multiple_of(m * 256, 256), 256)
                    acc[ms, :] += jnp.dot(hin[s, ms, :], w2in[s], preferred_element_type=jnp.float32)
                    return 0
                lax.fori_loop(0, toks // 256, mtile, 0)
            return 0
        lax.fori_loop(0, 2, block, 0)

    pair_a = (2 * yy, 2 * yy + 1)
    pair_b = (2 - 2 * yy, 3 - 2 * yy)

    def w2_local(j):
        p_arrive(1, j)

    def w2_remote(j):
        x_arrive(1, j)

    def mat2x(j):
        @pl.when(inner)
        def _():
            rcopy(w2x.at[j], w2x.at[j], wxs.at[j, 0], wxr.at[j], partner).wait_recv()
            a = pltpu.make_async_copy(w2x.at[j], w2in.at[0], msem.at[0, 0])
            b = pltpu.make_async_copy(hg.at[moved, j], hin.at[0], msem.at[0, 1])
            a.start()
            b.start()
            a.wait()
            b.wait()

            def mtile(m, _):
                ms = pl.ds(pl.multiple_of(m * 256, 256), 256)
                accx[ms, :] += jnp.dot(hin[0, ms, :], w2in[0], preferred_element_type=jnp.float32)
                return 0
            lax.fori_loop(0, toks // 256, mtile, 0)

    def start_wx2(j):
        @pl.when(jnp.logical_and(end, row == far))
        def _():
            wx2_desc(j, True).start()

        @pl.when(jnp.logical_and(end, row != far))
        def _():
            wx2_desc(j, False).start()

    def mat2y(j):
        i = EXTRA.index(j)

        @pl.when(inner)
        def _():
            rcopy(w2y.at[i], w2y.at[i], wx2s.at[i], wx2r.at[i], partner).wait_recv()
            a = pltpu.make_async_copy(w2y.at[i], w2in.at[0], msem.at[0, 0])
            b = pltpu.make_async_copy(hg.at[far, j], hin.at[0], msem.at[0, 1])
            a.start()
            b.start()
            a.wait()
            b.wait()

            def mtile(m, _):
                ms = pl.ds(pl.multiple_of(m * 256, 256), 256)
                accx[ms, :] += jnp.dot(hin[0, ms, :], w2in[0], preferred_element_type=jnp.float32)
                return 0
            lax.fori_loop(0, toks // 256, mtile, 0)

    def px_start():
        @pl.when(inner)
        def _():
            for m in range(2):
                px_desc(m).start()

    def px_finish():
        @pl.when(inner)
        def _():
            for m in range(2):
                px_desc(m).wait_recv()

                def add(i, _):
                    a = pl.ds(pl.multiple_of(m * hrow + c * mbt + i * 64, 64), 64)
                    b = pl.ds(pl.multiple_of(m * mbt + i * 64, 64), 64)
                    partx[b, :] += accx[a, :]
                    return 0
                lax.fori_loop(0, mbt // 64, add, 0)
            pe_desc().start()

    start_w(0)
    zero()
    events = dict(
        own=own_x_send, x=xhop, xd=x_done, g=gamma_done, ln=norm, y=y_arrive_forward, w=start_w,
        wx=lambda j: start_wx((j,)), wy=start_wx2, p=w1_ready, q=w2_local, r=w2_remote, f=mat1, h=hop,
        e=lambda j, m: hop(1, j, m, from_end=True),
        a=functools.partial(mat2, pair_a), b=functools.partial(mat2, pair_b), c=mat2x, d=mat2y,
        ps=px_start, pf=px_finish)
    for code in ORDER:
        name, *index = code.split("_")
        events[name](*map(int, index))
    def fin_desc(m):
        return rcopy(acc.at[pl.ds(m * hrow + (1 - c) * mbt, mbt), :], part.at[pl.ds(m * mbt, mbt), :],
                     fs.at[m], fr.at[m], partner)
    for m in range(2):
        fin_desc(m).start()

    @pl.when(end)
    def _():
        pe_desc().wait_recv()

        def add(i, _):
            for m in range(2):
                a = pl.ds(pl.multiple_of(m * hrow + c * mbt + i * 64, 64), 64)
                b = pl.ds(pl.multiple_of(m * mbt + i * 64, 64), 64)
                acc[a, :] += parte[b, :]
            return 0
        lax.fori_loop(0, mbt // 64, add, 0)

    for m in range(2):
        fin_desc(m).wait()

        def final(i, _):
            a = pl.ds(pl.multiple_of(m * hrow + c * mbt + i * 64, 64), 64)
            b = pl.ds(pl.multiple_of(m * mbt + i * 64, 64), 64)
            y_ref[b, :] = (xres[b, :].astype(jnp.float32) + (acc[a, :] + part[b, :])).astype(jnp.bfloat16)
            return 0
        lax.fori_loop(0, mbt // 64, final, 0)

    for w in range(2):
        def drain(j, _):
            p_desc(w, j).wait_send()
            for ct in range(2):
                y_desc(w, j, ct).wait_send()
            x_sent(w, j)
            return 0
        lax.fori_loop(0, NCHUNK, drain, 0)
    for k in range(3):
        rcopy(gamma_ref, gg.at[z], gs.at[k], gr.at[z], zoth[k]).wait_send()

    def drain_z(zz, _):
        for m in range(2):
            x_part(zz, m).wait_send()

        @pl.when(jnp.logical_and(zz <= z, z < 3))
        def _():
            for m in range(2):
                x_up(zz, m).wait_send()

        @pl.when(jnp.logical_and(zz >= z, z > 0))
        def _():
            for m in range(2):
                x_dn(zz, m).wait_send()

        for j in range(NCHUNK):
            @pl.when(jnp.logical_and(zz <= z, goes_up(zz, j)))
            def _():
                for m in range(2):
                    h_up(zz, j, m).wait_send()

            @pl.when(jnp.logical_and(zz >= z, goes_dn(zz, j)))
            def _():
                for m in range(2):
                    h_dn(zz, j, m).wait_send()
        return 0
    lax.fori_loop(0, 4, drain_z, 0)

    @pl.when(jnp.logical_and(end, row == moved))
    def _():
        def d(j, _):
            for ct in range(2):
                wx_desc(j, ct).wait_send()
            return 0
        lax.fori_loop(0, NCHUNK, d, 0)

    @pl.when(end)
    def _():
        for j in EXTRA:
            wx2_desc(j, False).wait_send()

    @pl.when(inner)
    def _():
        for m in range(2):
            px_desc(m).wait_send()
        pe_desc().wait_send()


def solution(mesh):
    act_spec = P(None, ("dp", "row"), "col")

    def per_device(x_blk, gamma_blk, w_in_blk, w_out_blk):
        mb, rows, dblk = x_blk.shape
        tok = mb * rows
        fz = w_in_blk.shape[1]
        fhalf = fz // 2
        nc = fhalf // NCHUNK
        bf16, f32 = jnp.bfloat16, jnp.float32
        x2 = x_blk.reshape(tok, dblk)
        g2 = jnp.broadcast_to(gamma_blk[None, :], (8, dblk))
        dma = pltpu.SemaphoreType.DMA
        anyspec = pl.BlockSpec(memory_space=pl.ANY)
        out = pl.pallas_call(
            _kernel,
            out_shape=(
                jax.ShapeDtypeStruct((tok, dblk), bf16),
                jax.ShapeDtypeStruct((NCHUNK, 4, w_in_blk.shape[0], nc), bf16),
                jax.ShapeDtypeStruct((4, NCHUNK, nc, dblk), bf16),
                jax.ShapeDtypeStruct((4, NCHUNK, 2 * tok, nc), bf16),
                jax.ShapeDtypeStruct((NCHUNK, nc, dblk), bf16),
                jax.ShapeDtypeStruct((max(len(EXTRA), 1), nc, dblk), bf16),
            ),
            in_specs=[anyspec] * 4,
            out_specs=(pl.BlockSpec(memory_space=pltpu.VMEM), anyspec, anyspec, anyspec, anyspec, anyspec),
            scratch_shapes=[
                pltpu.VMEM((4, 2 * tok, dblk), bf16),
                pltpu.VMEM((2 * tok, 4 * dblk), bf16),
                pltpu.VMEM((4, 8, dblk), f32),
                pltpu.VMEM((2, 4 * dblk, 256), bf16),
                pltpu.VMEM((2 * tok, nc), bf16),
                pltpu.VMEM((2 * tok, dblk), f32),
                pltpu.VMEM((2 * tok, dblk), f32),
                pltpu.VMEM((2, 2 * tok, nc), bf16),
                pltpu.VMEM((2, nc, dblk), bf16),
                pltpu.VMEM((tok, dblk), f32),
                pltpu.VMEM((tok, dblk), f32),
                pltpu.VMEM((tok, dblk), f32),
                pltpu.VMEM((tok, dblk), bf16),
                dma((2, NCHUNK, 2)), dma((2, NCHUNK, 2)), dma((2, NCHUNK, 2)), dma((2, NCHUNK, 2)),
                dma((2, NCHUNK)), dma((2, NCHUNK)),
                dma((4, 2)), dma((4, 2)), dma((4, 2)), dma((4, 2)), dma((4, 2)), dma((3,)), dma((4,)),
                dma((4, NCHUNK, 2)), dma((4, NCHUNK, 2)), dma((4, NCHUNK, 2)), dma((2,)), dma((2,)),
                dma((NCHUNK, 2)), dma((NCHUNK,)), dma((max(len(EXTRA), 1),)), dma((max(len(EXTRA), 1),)),
                dma((2,)), dma((2,)), dma, dma,
                dma((4,)), dma((2, 4)), dma((1,)), dma((2, 2)),
            ],
            compiler_params=pltpu.CompilerParams(
                collective_id=0, has_side_effects=True, vmem_limit_bytes=66_000_000),
            name="mlp",
        )(x2, g2, w_in_blk, w_out_blk)
        return out[0].reshape(mb, rows, dblk)

    return jax.shard_map(
        per_device, mesh=mesh, in_specs=(act_spec, P("col"), P("row", "col"), P("row", "col")),
        out_specs=act_spec, check_vma=False)
```
